32 devices in a mesh: seq: 8 (over y, x, core), head: 4 (over z).
Axes of the slice: x: 2, y: 2, z: 4, core: 2. Of those that a mesh axis runs over, the one named last changes fastest.
Arguments:
- queries: bfloat16 [4096, 1024], P('seq', 'head'), may hold values from -16 to 16
- keys: bfloat16 [4096, 1024], P('seq', 'head'), may hold values from -16 to 16
- values: bfloat16 [4096, 1024], P('seq', 'head'), may hold values from -6 to 6
- segment_ids: int32 [4096], P('seq'), may hold values from 0 to 4, never falling along the last dimension, each value on 1 to 1024 neighbouring positions
- out_weight: bfloat16 [1024, 5120], P('head'), may hold values from -0.25 to 0.25
Outputs:
- mixed: bfloat16 [4096, 5120], P('seq', 'head')
The draws below stay inside these ranges and needn't reach their ends.
Inputs may be any that keep to these rules, and one draw needn't show every extreme that they name: `segment_ids`: segment numbers never fall along the sequence; a segment holds at most 1024 tokens.
All inputs are finite; a program needn't handle non-finite values.
Results may differ from the reference program's by a relative error of at most 0.02.
Values may be sent and summed in bfloat16 or wider, within the bound.
No kernel may reach another device: no remote copies, remote signals or barrier semaphores. Data moves between devices by JAX's collectives and lax.ppermute only.
A program may use at most 64 MiB of HBM per device.

```python
import math
import jax
import jax.numpy as jnp
import numpy as np
from jax import lax

D = 5120
HD = 128
HEAD_DEV = 2
TOK_DEV = 512
SPAN = 2
HEADS = 8
TOKENS = 4096
SEG_MOST = 1024
N_SEQ = 8
N_HEAD = 4


def paired_draw(key):
    first, second = jax.random.split(jax.random.fold_in(key, 7), 2)
    shape = (TOKENS, HEADS * HD)
    query = jnp.clip(jax.random.normal(first, shape, jnp.float32), -6.0, 6.0)
    keyrow = jnp.clip(jax.random.normal(second, shape, jnp.float32), -6.0, 6.0)
    return (query, keyrow)


def draw_queries(key, part):
    return paired_draw(key)[0].astype(jnp.bfloat16)


def draw_keys(key, part):
    return paired_draw(key)[1].astype(jnp.bfloat16)


def with_spikes(values, key, source, target, shards_of, factor):
    owner, partner = [(jnp.arange(values.shape[axis_at]) // (values.shape[axis_at] // shards_of)).reshape([-1 if axis == axis_at else 1 for axis in range(values.ndim)]) for axis_at in (source, target)]
    chosen = jax.random.permutation(key, shards_of)[partner]
    strong = (owner == chosen) | (owner == (partner + shards_of // 2) % shards_of)
    return jnp.where(strong, factor * values, values)


def shard_levels(own_key, shape, cuts, low, top_value):
    factor_of = 1.0
    for dim, parts in cuts:
        draws = jax.random.uniform(jax.random.fold_in(jax.random.fold_in(own_key, 6), dim), (parts,), jnp.float32, low / len(cuts), top_value / len(cuts))
        factor_of = factor_of * jnp.repeat(jnp.exp(draws), shape[dim] // parts).reshape((-1,) + (1,) * (len(shape) - 1 - dim))
    return factor_of


def split_up(number_of, total, most, slope):
    loads = [(1 << 20) // math.isqrt(grade ** slope) + 1 for grade in range(2, number_of + 1)]
    surplus, holding = total - most - (number_of - 1), [1] * (number_of - 1)
    while surplus > 0:
        free = [i for i in range(number_of - 1) if holding[i] < most]
        mass, left = sum([loads[i] for i in free]), surplus
        for i in free:
            extra = min(most - holding[i], max(1, left * loads[i] // mass), surplus)
            holding[i] = holding[i] + extra
            surplus = surplus - extra
    return np.array([most] + holding)


def ragged_sizes(rng, count, total, bound, lean):
    if count == 2:
        one = jax.random.randint(rng, (), max(1, total - bound), min(bound, total - 1) + 1)
        return jnp.stack([one, total - one])
    tallies = jnp.asarray(split_up(count, total, bound, lean), jnp.int32)
    couples = (count - 1) // 2
    donor, sink = tallies[1:1 + 2 * couples:2], tallies[2:2 + 2 * couples:2]
    room = jnp.minimum(donor - 1, bound - sink)
    moved = jax.random.randint(jax.random.fold_in(rng, 1), (couples,), 0, 1 << 20) % (room + 1)
    tallies = tallies.at[1:1 + 2 * couples:2].set(donor - moved).at[2:2 + 2 * couples:2].set(sink + moved)
    return tallies[jax.random.permutation(jax.random.fold_in(rng, 2), count)]


def normal_values(stream_key, extent, scale, most, shards=(), held_as=jnp.bfloat16):
    result = scale * jax.random.normal(stream_key, extent, jnp.float32)
    if shards:
        result = result * shard_levels(stream_key, extent, shards, -0.22, 0.18)
    return jnp.clip(result, -most, most).astype(held_as)


def noise_with(key, extent, scale, most, cuts, heavy, held_as=jnp.bfloat16):
    entries = scale * jax.random.normal(key, extent, jnp.float32)
    if cuts:
        entries = entries * shard_levels(key, extent, cuts, -0.22, 0.18)
    return jnp.clip(with_spikes(entries, jax.random.fold_in(key, 3), *heavy), -most, most).astype(held_as)


def setup_inputs(seed: int = 0) -> dict:
    arg_keys = jax.random.split(jax.random.key(seed), 6)
    queries = draw_queries(jax.random.fold_in(arg_keys[5], 71), 0)
    keys = draw_keys(jax.random.fold_in(arg_keys[5], 71), 0)
    values = normal_values(arg_keys[2], (TOKENS, HEADS * HD), 1.0, 6.0, ((0, 8), (1, 4)))
    segment_ids = jnp.searchsorted(jnp.cumsum(ragged_sizes(arg_keys[3], 2 * N_SEQ // 3, TOKENS, SEG_MOST, 1)), jnp.arange(TOKENS), side="right").astype(jnp.int32)
    out_weight = noise_with(arg_keys[4], (HEADS * HD, D), (HEADS * HD) ** -0.5, 0.25, ((0, 4),), (0, 1, 4, 2.0))
    return {"queries": queries, "keys": keys, "values": values, "segment_ids": segment_ids, "out_weight": out_weight}


def reference(queries, keys, values, segment_ids, out_weight):
    width = HEADS * HD
    pad = SPAN * TOK_DEV
    keys_pad = jnp.concatenate([jnp.zeros((pad, width), keys.dtype), keys, jnp.zeros((pad, width), keys.dtype)], axis=0)
    values_pad = jnp.concatenate([jnp.zeros((pad, width), values.dtype), values, jnp.zeros((pad, width), values.dtype)], axis=0)
    neg = -jnp.ones((pad,), jnp.int32)
    seg_pad = jnp.concatenate([neg, segment_ids.astype(jnp.int32), neg], axis=0)
    window = (2 * SPAN + 1) * TOK_DEV

    def block(index):
        start = (index * TOK_DEV).astype(jnp.int32)
        query = lax.dynamic_slice_in_dim(queries, start, TOK_DEV, 0).astype(jnp.float32).reshape(TOK_DEV, HEADS, HD)
        qseg = lax.dynamic_slice_in_dim(segment_ids.astype(jnp.int32), start, TOK_DEV, 0)
        near_k = lax.dynamic_slice_in_dim(keys_pad, start, window, 0).astype(jnp.float32).reshape(window, HEADS, HD)
        near_v = lax.dynamic_slice_in_dim(values_pad, start, window, 0).astype(jnp.float32).reshape(window, HEADS, HD)
        kseg = lax.dynamic_slice_in_dim(seg_pad, start, window, 0)
        scores = jnp.einsum("qhd,khd->hqk", query, near_k) * (HD ** -0.5)
        allowed = (qseg[:, None] == kseg[None, :])[None]
        scores = jnp.where(allowed, scores, -1e30)
        peak = jnp.max(scores, axis=2)
        weights = jnp.where(allowed, jnp.exp(scores - peak[:, :, None]), 0.0)
        total = jnp.sum(weights, axis=2)
        rounded = lax.optimization_barrier(weights.astype(jnp.bfloat16)).astype(jnp.float32)
        summed = jnp.einsum("hqk,khd->qhd", rounded, near_v)
        attended = summed / jnp.transpose(total)[:, :, None]
        return attended.reshape(TOK_DEV, width).astype(jnp.bfloat16)

    attended = lax.map(block, jnp.arange(N_SEQ, dtype=jnp.int32)).reshape(TOKENS, width)
    group = HEAD_DEV * HD
    mixed = jnp.zeros((TOKENS, D), jnp.float32)
    for index in range(N_HEAD):
        term = jnp.dot(attended[:, index * group:(index + 1) * group], out_weight[index * group:(index + 1) * group], preferred_element_type=jnp.float32)
        mixed = mixed + term.astype(jnp.bfloat16).astype(jnp.float32)
    return mixed.astype(jnp.bfloat16)
```

```python
import functools
import math

import jax
import jax.numpy as jnp
from jax import lax
from jax.experimental import pallas as pl
from jax.experimental.pallas import tpu as pltpu
from jax.sharding import PartitionSpec as P

HEAD_DEV = 2
QUERY_TILE = 128
PAD_ROWS = 16


def whole(shape):
    return pl.BlockSpec(shape, lambda *_: (0,) * len(shape))


def rotate(block, axis, distance):
    count = lax.axis_size(axis)
    return lax.ppermute(block, axis, [(i, (i + distance) % count) for i in range(count)])


def shifted(block, axis, distance):
    devices = range(lax.axis_size(axis))
    return lax.ppermute(block, axis, [(i - distance, i) for i in devices if i - distance in devices])


def exchanged(block, axis, flip):
    return lax.ppermute(block, axis, [(i, i ^ flip) for i in range(lax.axis_size(axis))])


def pack(keys, values, marks):
    rows, width = keys.shape
    head = width // HEAD_DEV
    mark_rows = marks.shape[0]

    def body(k_ref, v_ref, m_ref, first_ref, *rest):
        for index, ref in enumerate((first_ref, *rest)):
            part = slice(index * head, (index + 1) * head)
            ref[:rows, :head] = k_ref[:, part]
            ref[:rows, head:] = v_ref[:, part]
        tail = jnp.zeros((PAD_ROWS - mark_rows, 2 * head), jnp.float32)
        first_ref[rows:, :] = jnp.concatenate([m_ref[...], tail], axis=0).astype(jnp.bfloat16)

    shapes = [(rows + PAD_ROWS, 2 * head)] + [(rows, 2 * head)] * (HEAD_DEV - 1)
    return pl.pallas_call(
        body,
        name="pack",
        out_shape=[jax.ShapeDtypeStruct(shape, jnp.bfloat16) for shape in shapes],
        cost_estimate=pl.CostEstimate(flops=0, bytes_accessed=8 * rows * width, transcendentals=0),
    )(keys, values, marks)


def attend(query, query_marks, blocks, mark_blocks, index):
    rows = query.shape[0]
    head = query.shape[1] // HEAD_DEV
    count = len(blocks)
    mark_rows = rows // (2 * head)
    span = count * rows
    scale = head ** -0.5 * math.log2(math.e)

    def body(q_ref, qm_ref, *refs):
        block_refs = refs[:count]
        mark_refs = refs[count:2 * count]
        out_ref = refs[2 * count]
        for start in range(0, rows, QUERY_TILE):
            tile = slice(start, start + QUERY_TILE)
            q_tile = q_ref[tile, :]
            q_mark = qm_ref[tile, :]
            q_mark = jnp.concatenate([q_mark] * (2 * head // q_mark.shape[1]), axis=1)
            parts = []
            for block, mark in zip(block_refs, mark_refs):
                for piece in range(mark_rows):
                    lines = slice(piece * 2 * head, (piece + 1) * 2 * head)
                    score = lax.dot_general(
                        q_tile, block[lines, :head], (((1,), (1,)), ((), ())),
                        preferred_element_type=jnp.float32,
                    )
                    row = mark[piece:piece + 1, :].astype(jnp.float32)
                    parts.append(jnp.where(q_mark == row, score, -1e30))
            peak = functools.reduce(jnp.maximum, parts)
            peak = jnp.max(peak, axis=1, keepdims=True)
            weights = [jnp.exp2((part - peak) * scale) for part in parts]
            total = jnp.sum(functools.reduce(jnp.add, weights), axis=1, keepdims=True)
            summed = jnp.zeros((QUERY_TILE, head), jnp.float32)
            step = 0
            for block in block_refs:
                for piece in range(mark_rows):
                    lines = slice(piece * 2 * head, (piece + 1) * 2 * head)
                    summed += jnp.dot(
                        weights[step].astype(jnp.bfloat16), block[lines, head:],
                        preferred_element_type=jnp.float32,
                    )
                    step += 1
            out_ref[tile, :] = (summed / total).astype(jnp.bfloat16)

    return pl.pallas_call(
        body,
        name="attend",
        grid=(1,),
        in_specs=[
            pl.BlockSpec((rows, head), lambda i: (0, index)),
            whole(query_marks.shape),
            *[pl.BlockSpec((rows, 2 * head), lambda i: (0, 0)) for _ in blocks],
            *[pl.BlockSpec((PAD_ROWS, 2 * head), lambda i: (rows // PAD_ROWS, 0)) for _ in mark_blocks],
        ],
        out_specs=whole((rows, head)),
        out_shape=jax.ShapeDtypeStruct((rows, head), jnp.bfloat16),
        cost_estimate=pl.CostEstimate(
            flops=8 * rows * span * head, bytes_accessed=4 * span * head, transcendentals=rows * span
        ),
    )(query, query_marks, *blocks, *mark_blocks)


def assemble(order, pieces):
    groups, part, columns = pieces[0].shape
    count = len(pieces)

    def body(order_ref, *refs):
        out_ref = refs[-1]
        for index, ref in enumerate(refs[:-1]):
            place = pl.multiple_of((order_ref[0] ^ index) * part, part)
            out_ref[:, pl.ds(place, part), :] = ref[...]

    return pl.pallas_call(
        body,
        name="assemble",
        in_specs=[pl.BlockSpec(memory_space=pltpu.SMEM)] + [pl.BlockSpec(memory_space=pltpu.VMEM)] * count,
        out_shape=jax.ShapeDtypeStruct((groups, part * count, columns), jnp.bfloat16),
        cost_estimate=pl.CostEstimate(
            flops=0, bytes_accessed=4 * groups * part * count * columns, transcendentals=0
        ),
    )(order, *pieces)


def gathered_weight(out_weight, axis):
    groups = lax.axis_size(axis)
    replicas = 4
    rows, width = out_weight.shape
    part, columns = rows // replicas, width // groups
    me = lax.axis_index(axis)
    place = lax.axis_index("seq")
    mine = (place & 1) + 2 * ((place >> 2) & 1)
    received = []
    for distance in range(1, groups):
        target = (me + distance) % groups
        piece = lax.dynamic_slice(out_weight, (mine * part, target * columns), (part, columns))
        received.append(rotate(piece, axis, distance))
    first = jnp.stack(received)
    second = exchanged(first, "seq", 4)
    near = exchanged(jnp.stack([first, second]), "seq", 1)
    others = assemble(mine.astype(jnp.int32)[None], [first, near[0], second, near[1]])
    own = lax.dynamic_slice(out_weight, (0, me * columns), (rows, columns))
    return own, others


def shards(queries, keys, values, segment_ids, out_weight):
    rows, width = queries.shape
    head = width // HEAD_DEV
    groups = lax.axis_size("head")
    marks = (segment_ids + 1).astype(jnp.float32)
    query_marks = jnp.broadcast_to(marks[:, None], (rows, head))
    messages = pack(keys, values, marks.reshape(rows // (2 * head), 2 * head))
    even = lax.axis_index("seq") % 2 == 0

    own_weight, other_weight = gathered_weight(out_weight, "head")

    mark_blocks = None
    sent = []
    for index, message in enumerate(messages):
        left = shifted(message, "seq", 2)
        right = shifted(message, "seq", -2)
        beside = exchanged(message, "seq", 1)
        across = exchanged(jnp.where(even, right, left), "seq", 1)
        blocks = (message, beside, left, right, across)
        if mark_blocks is None:
            mark_blocks = blocks
        done = attend(queries, query_marks, blocks, mark_blocks, index)
        sent.append([done] + [rotate(done, "head", distance) for distance in range(1, groups)])

    mixed = jnp.zeros((rows, own_weight.shape[1]), jnp.float32)
    for distance in range(groups):
        weight = own_weight if distance == 0 else other_weight[distance - 1]
        group = jnp.concatenate([part[distance] for part in sent], axis=1)
        mixed += jnp.dot(group, weight, preferred_element_type=jnp.float32)
    return mixed.astype(jnp.bfloat16)


def solution(mesh):
    placed = (P("seq", "head"), P("seq", "head"), P("seq", "head"), P("seq"), P("head", None))
    return jax.shard_map(
        shards, mesh=mesh, in_specs=placed, out_specs=P("seq", "head"), check_vma=False
    )
```

```python
import functools
import math

import jax
import jax.numpy as jnp
from jax import lax
from jax.experimental import pallas as pl
from jax.experimental.pallas import tpu as pltpu
from jax.sharding import PartitionSpec as P

HEAD_DEV = 2
QUERY_TILE = 256
PAD_ROWS = 16
KERNEL_VMEM = 12 * 2**20
IN_VMEM = pl.BlockSpec(memory_space=pltpu.VMEM)


def partner(index, distance, count):
    return index ^ distance if count & (count - 1) == 0 else (index + distance) % count


def to_partner(block, axis, distance):
    count = lax.axis_size(axis)
    return lax.ppermute(block, axis, [(i, partner(i, distance, count)) for i in range(count)])


def relays():
    return ()


def exchanged(block, axis, flip):
    return lax.ppermute(block, axis, [(i, i ^ flip) for i in range(lax.axis_size(axis))])


def from_far(block, axis, toward):
    count = lax.axis_size(axis)
    route = [(i + toward * (2 if i % 2 == 0 else -2), i) for i in range(count)]
    return lax.ppermute(block, axis, [(s, d) for s, d in route if 0 <= s < count])


def pack(keys, values, segment_ids):
    rows, width = keys.shape
    head = width // HEAD_DEV
    wide = 2 * head
    lines = rows // wide

    def body(k_ref, v_ref, s_ref, column_ref, *refs):
        messages, (ids_ref, sems) = refs[:HEAD_DEV], refs[HEAD_DEV:]
        copies = [pltpu.make_async_copy(s_ref, ids_ref, sems.at[0])]
        for index, ref in enumerate(messages):
            for side, source in enumerate((k_ref, v_ref)):
                copies.append(pltpu.make_async_copy(
                    source.at[:, index * head:(index + 1) * head],
                    ref.at[:rows, side * head:(side + 1) * head],
                    sems.at[1 + 2 * index + side],
                ))
        for copy in copies:
            copy.start()
        copies[0].wait()
        marks = (ids_ref[...] + 1).astype(jnp.float32)
        parts = [marks[:, i * wide:(i + 1) * wide] for i in range(lines)]
        parts.append(jnp.zeros((PAD_ROWS - lines, wide), jnp.float32))
        messages[0][rows:, :] = jnp.concatenate(parts, axis=0).astype(jnp.bfloat16)
        column_ref[...] = jnp.transpose(jnp.broadcast_to(marks, (head, rows)))
        for copy in copies[1:]:
            copy.wait()

    shapes = [(rows + PAD_ROWS, wide)] + [(rows, wide)] * (HEAD_DEV - 1)
    return pl.pallas_call(
        body,
        name="pack",
        in_specs=[pl.BlockSpec(memory_space=pltpu.HBM)] * 3,
        out_specs=[IN_VMEM] * (1 + HEAD_DEV),
        out_shape=[jax.ShapeDtypeStruct((rows, head), jnp.float32)]
        + [jax.ShapeDtypeStruct(shape, jnp.bfloat16) for shape in shapes],
        scratch_shapes=[
            pltpu.VMEM((1, rows), jnp.int32), pltpu.SemaphoreType.DMA((1 + 2 * HEAD_DEV,)),
        ],
        compiler_params=pltpu.CompilerParams(vmem_limit_bytes=KERNEL_VMEM),
        cost_estimate=pl.CostEstimate(flops=10**9, bytes_accessed=8 * rows * width, transcendentals=0),
    )(*[pltpu.with_memory_space_constraint(x, pltpu.HBM) for x in (keys, values, segment_ids.reshape(1, rows))])


def attend(query, query_marks, blocks, index, marks=None):
    rows = query.shape[0]
    head = query.shape[1] // HEAD_DEV
    wide = 2 * head
    count = len(blocks)
    lines = rows // wide
    span = count * rows
    scale = head ** -0.5 * math.log2(math.e)
    first = marks is None
    kept = -(-count * lines // 8) * 8

    def body(*refs):
        q_ref, qm_ref = refs[:2]
        block_refs = refs[2:2 + count]
        if first:
            out_ref, marks_ref, score_ref = refs[2 + count:]
            pieces = [ref[rows:rows + lines, :].astype(jnp.float32) for ref in block_refs]
            pieces.append(jnp.zeros((kept - count * lines, wide), jnp.float32))
            marks_ref[...] = jnp.concatenate(pieces, axis=0)
        else:
            marks_ref, out_ref, score_ref = refs[2 + count:]
        for start in range(0, rows, QUERY_TILE):
            tile = slice(start, start + QUERY_TILE)
            q_tile = q_ref[tile, index * head:(index + 1) * head]
            q_mark = qm_ref[tile, :]
            q_mark = jnp.concatenate([q_mark] * 2, axis=1)
            peak = None
            for piece in range(count * lines):
                block, offset = block_refs[piece // lines], piece % lines * wide
                score = lax.dot_general(
                    q_tile, block[offset:offset + wide, :head], (((1,), (1,)), ((), ())),
                    preferred_element_type=jnp.float32,
                )
                score = jnp.where(q_mark == marks_ref[piece:piece + 1, :], score, -1e30)
                score_ref[:, piece * wide:(piece + 1) * wide] = score
                largest = jnp.maximum(score[:, :head], score[:, head:])
                peak = largest if peak is None else jnp.maximum(peak, largest)
            peak = jnp.max(peak, axis=1, keepdims=True)
            summed, total = None, None
            for piece in range(count * lines):
                block, offset = block_refs[piece // lines], piece % lines * wide
                weight = jnp.exp2((score_ref[:, piece * wide:(piece + 1) * wide] - peak) * scale)
                folded = weight[:, :head] + weight[:, head:]
                term = jnp.dot(
                    weight.astype(jnp.bfloat16), block[offset:offset + wide, head:],
                    preferred_element_type=jnp.float32,
                )
                total = folded if total is None else total + folded
                summed = term if summed is None else summed + term
            total = jnp.sum(total, axis=1, keepdims=True)
            out_ref[tile, :] = (summed / total).astype(jnp.bfloat16)

    outs = [jax.ShapeDtypeStruct((rows, head), jnp.bfloat16)]
    if first:
        outs.append(jax.ShapeDtypeStruct((kept, wide), jnp.float32))
    result = pl.pallas_call(
        body,
        name="attend",
        in_specs=[IN_VMEM] * (2 + count + (not first)),
        out_specs=[IN_VMEM] * len(outs),
        out_shape=outs,
        scratch_shapes=[pltpu.VMEM((QUERY_TILE, span), jnp.float32)],
        compiler_params=pltpu.CompilerParams(vmem_limit_bytes=KERNEL_VMEM),
        cost_estimate=pl.CostEstimate(
            flops=8 * rows * span * head, bytes_accessed=4 * span * head, transcendentals=rows * span
        ),
    )(query, query_marks, *blocks, *([] if first else [marks]))
    return result if first else (result[0], marks)


def assemble(order, own, pieces):
    groups, part, columns = pieces[0].shape
    count = len(pieces)

    def body(order_ref, own_ref, *refs):
        out_ref = refs[-1]
        out_ref[0] = own_ref[...]
        for index, ref in enumerate(refs[:-1]):
            place = pl.multiple_of((order_ref[0] ^ index) * part, part)
            out_ref[1:, pl.ds(place, part), :] = ref[...]

    return pl.pallas_call(
        body,
        name="assemble",
        in_specs=[pl.BlockSpec(memory_space=pltpu.SMEM)] + [IN_VMEM] * (count + 1),
        out_specs=IN_VMEM,
        out_shape=jax.ShapeDtypeStruct((groups + 1, part * count, columns), jnp.bfloat16),
        compiler_params=pltpu.CompilerParams(vmem_limit_bytes=KERNEL_VMEM),
        cost_estimate=pl.CostEstimate(
            flops=10**9, bytes_accessed=4 * groups * part * count * columns, transcendentals=0
        ),
    )(order, own, *pieces)


def tiles(columns):
    tile = 256 if columns % 256 == 0 else columns
    return [slice(start, start + tile) for start in range(0, columns, tile)]


def placed(left_ref, refs, parts):
    place = 0
    refs = iter(refs)
    for arrays in parts:
        value = functools.reduce(jnp.add, [next(refs)[...] for _ in arrays])
        left_ref[:, place:place + value.shape[1]] = value
        place += value.shape[1]


def project_first(weight, own, others):
    groups, depth, columns = weight.shape
    rows, head = own[0].shape
    parts = [[array] for array in own] + others
    flat = [array for arrays in parts for array in arrays]

    def body(w_ref, *refs):
        ins, out_ref, left_ref = refs[:len(flat)], refs[-2], refs[-1]
        placed(left_ref, ins, parts)
        for tile in tiles(columns):
            out = jnp.dot(left_ref[:, :depth], w_ref[0, :, tile], preferred_element_type=jnp.float32)
            for g in range(1, groups):
                place = depth + (g - 1) * head
                out += jnp.dot(
                    left_ref[:, place:place + head], w_ref[g, :head, tile],
                    preferred_element_type=jnp.float32,
                )
            out_ref[:, tile] = out

    return pl.pallas_call(
        body,
        name="project_first",
        in_specs=[IN_VMEM] * (1 + len(flat)),
        out_specs=IN_VMEM,
        out_shape=jax.ShapeDtypeStruct((rows, columns), jnp.float32),
        scratch_shapes=[pltpu.VMEM((rows, depth + (groups - 1) * head), jnp.bfloat16)],
        compiler_params=pltpu.CompilerParams(vmem_limit_bytes=KERNEL_VMEM),
        cost_estimate=pl.CostEstimate(
            flops=rows * groups * depth * columns, bytes_accessed=4 * columns * rows, transcendentals=0
        ),
    )(weight, *flat)


def project_last(weight, partial, others):
    groups, depth, columns = weight.shape
    rows, head = others[0][0].shape
    flat = [array for arrays in others for array in arrays]
    span = (groups - 1) * (depth - head)
    cuts = tiles(columns)

    def body(w_ref, p_ref, *refs):
        ins, (out_ref, left_ref, right_ref, done_ref, sems) = refs[:len(flat)], refs[len(flat):]
        placed(left_ref, ins, others)
        for g in range(1, groups):
            place = (g - 1) * (depth - head)
            right_ref[place:place + depth - head, :] = w_ref[g, head:, :]
        copies = []
        for number, tile in enumerate(cuts):
            out = p_ref[:, tile] + jnp.dot(
                left_ref[...], right_ref[:, tile], preferred_element_type=jnp.float32
            )
            done_ref[:, tile] = out.astype(jnp.bfloat16)
            copies.append(pltpu.make_async_copy(done_ref.at[:, tile], out_ref.at[:, tile], sems.at[number]))
            copies[-1].start()
        for copy in copies:
            copy.wait()

    return pl.pallas_call(
        body,
        name="project_last",
        in_specs=[IN_VMEM] * (2 + len(flat)),
        out_specs=pl.BlockSpec(memory_space=pltpu.HBM),
        out_shape=jax.ShapeDtypeStruct((rows, columns), jnp.bfloat16),
        scratch_shapes=[
            pltpu.VMEM((rows, span), jnp.bfloat16),
            pltpu.VMEM((span, columns), jnp.bfloat16),
            pltpu.VMEM((rows, columns), jnp.bfloat16),
            pltpu.SemaphoreType.DMA((len(cuts),)),
        ],
        compiler_params=pltpu.CompilerParams(vmem_limit_bytes=2 * KERNEL_VMEM),
        cost_estimate=pl.CostEstimate(
            flops=rows * groups * depth * columns, bytes_accessed=4 * columns * rows, transcendentals=0
        ),
    )(weight, partial, *flat)


def shards(queries, keys, values, segment_ids, out_weight):
    groups = lax.axis_size("head")
    me = lax.axis_index("head")
    place = lax.axis_index("seq")
    replicas = 4
    mine = (place & 1) + 2 * ((place >> 2) & 1)
    part, columns = out_weight.shape[0] // replicas, out_weight.shape[1] // groups

    query_marks, *messages = pack(keys, values, segment_ids)

    near, far, beside = [], [], []
    for message in messages:
        near.append(from_far(message, "seq", 1))
        far.append(from_far(message, "seq", -1))
        beside.append(exchanged(message, "seq", 1))

    received = []
    for distance in range(1, groups):
        target = partner(me, distance, groups)
        piece = lax.dynamic_slice(out_weight, (mine * part, target * columns), (part, columns))
        received.append(to_partner(piece, "head", distance))
    first = jnp.stack(received)
    second = exchanged(first, "seq", 4)
    third = exchanged(first, "seq", 1)
    fourth = exchanged(second, "seq", 1)
    own = lax.dynamic_slice(out_weight, (0, me * columns), (out_weight.shape[0], columns))
    weight = assemble(mine.astype(jnp.int32)[None], own, [first, third, second, fourth])

    own, others, marks = [], [], None
    for index, message in enumerate(messages):
        across = exchanged(near[index], "seq", 1)
        blocks = (message, beside[index], near[index], far[index], across)
        done, marks = attend(queries, query_marks, blocks, index, marks)
        own.append(done)
        if index in relays():
            two = lax.ppermute(done, "head", [(0, 2), (2, 0), (1, 3), (3, 1)])
            one = lax.ppermute(done, "head", [(0, 1), (1, 0), (2, 3), (3, 2)])
            inner = lax.ppermute(done, "head", [(1, 2), (2, 1)])
            outer = lax.ppermute(two, "head", [(1, 0), (2, 3)])
            others.append([[one], [two], [inner, outer]])
        else:
            line = []
            for distance in range(1, groups):
                line.append([to_partner(done, "head", distance)])
            others.append(line)

    partial = project_first(weight, own, others[0])
    rest = [line[distance] for distance in range(groups - 1) for line in others[1:]]
    return project_last(weight, partial, rest)


def solution(mesh):
    placed = (P("seq", "head"), P("seq", "head"), P("seq", "head"), P("seq"), P("head", None))
    return jax.shard_map(shards, mesh=mesh, in_specs=placed, out_specs=P("seq", "head"), check_vma=False)
```

```python
import functools
import math

import jax
import jax.numpy as jnp
from jax import lax
from jax.experimental import pallas as pl
from jax.experimental.pallas import tpu as pltpu
from jax.sharding import PartitionSpec as P

HEAD_DEV = 2
QUERY_TILE = 256
PAD_ROWS = 16
KERNEL_VMEM = 12 * 2**20
IN_VMEM = pl.BlockSpec(memory_space=pltpu.VMEM)
IN_HBM = pl.BlockSpec(memory_space=pltpu.HBM)
LANES = 128


def in_hbm(array):
    return pltpu.with_memory_space_constraint(array, pltpu.HBM)


def partner(index, distance, count):
    return index ^ distance if count & (count - 1) == 0 else (index + distance) % count


def to_partner(block, axis, distance):
    count = lax.axis_size(axis)
    return lax.ppermute(block, axis, [(i, partner(i, distance, count)) for i in range(count)])


def relays():
    return ()


def exchanged(block, axis, flip):
    return lax.ppermute(block, axis, [(i, i ^ flip) for i in range(lax.axis_size(axis))])


def from_far(block, axis, toward):
    count = lax.axis_size(axis)
    route = [(i + toward * (2 if i % 2 == 0 else -2), i) for i in range(count)]
    return lax.ppermute(block, axis, [(s, d) for s, d in route if 0 <= s < count])


def pack(keys, values, segment_ids):
    rows, width = keys.shape
    head = width // HEAD_DEV
    wide = 2 * head
    lines = rows // wide

    def body(k_ref, v_ref, s_ref, *refs):
        messages, (ids_ref, sems) = refs[:HEAD_DEV], refs[HEAD_DEV:]
        copies = [pltpu.make_async_copy(s_ref, ids_ref, sems.at[0])]
        for index, ref in enumerate(messages):
            for side, source in enumerate((k_ref, v_ref)):
                copies.append(pltpu.make_async_copy(
                    source.at[:, index * head:(index + 1) * head],
                    ref.at[:rows, side * head:(side + 1) * head],
                    sems.at[1 + 2 * index + side],
                ))
        for copy in copies:
            copy.start()
        copies[0].wait()
        marks = (ids_ref[...] + 1).astype(jnp.float32)
        parts = [marks[:, i * wide:(i + 1) * wide] for i in range(lines)]
        parts.append(jnp.zeros((PAD_ROWS - lines, wide), jnp.float32))
        messages[0][rows:, :] = jnp.concatenate(parts, axis=0).astype(jnp.bfloat16)
        for copy in copies[1:]:
            copy.wait()

    shapes = [(rows + PAD_ROWS, wide)] + [(rows, wide)] * (HEAD_DEV - 1)
    return pl.pallas_call(
        body,
        name="pack",
        in_specs=[IN_HBM] * 3,
        out_specs=[IN_VMEM] * HEAD_DEV,
        out_shape=[jax.ShapeDtypeStruct(shape, jnp.bfloat16) for shape in shapes],
        scratch_shapes=[
            pltpu.VMEM((1, rows), jnp.int32), pltpu.SemaphoreType.DMA((1 + 2 * HEAD_DEV,)),
        ],
        compiler_params=pltpu.CompilerParams(vmem_limit_bytes=KERNEL_VMEM),
        cost_estimate=pl.CostEstimate(flops=10**9, bytes_accessed=8 * rows * width, transcendentals=0),
    )(*[in_hbm(x) for x in (keys, values, segment_ids.reshape(1, rows))])


def cut(array, corners, rows, columns):
    count = corners.shape[0] // 2

    def body(corner_ref, source_ref, *refs):
        copies = []
        for index in range(count):
            row = pl.multiple_of(corner_ref[2 * index], rows)
            column = pl.multiple_of(corner_ref[2 * index + 1], columns)
            copies.append(pltpu.make_async_copy(
                source_ref.at[pl.ds(row, rows), pl.ds(column, columns)], refs[index], refs[-1].at[index]
            ))
        for copy in copies:
            copy.start()
        for copy in copies:
            copy.wait()

    return pl.pallas_call(
        body,
        name="cut",
        in_specs=[pl.BlockSpec(memory_space=pltpu.SMEM), IN_HBM],
        out_specs=[IN_VMEM] * count,
        out_shape=[jax.ShapeDtypeStruct((rows, columns), array.dtype)] * count,
        scratch_shapes=[pltpu.SemaphoreType.DMA((count,))],
        compiler_params=pltpu.CompilerParams(vmem_limit_bytes=KERNEL_VMEM),
        cost_estimate=pl.CostEstimate(
            flops=10**9, bytes_accessed=4 * count * rows * columns, transcendentals=0
        ),
    )(corners, in_hbm(array))


def stacked(arrays):
    def body(*refs):
        for index, ref in enumerate(refs[:-1]):
            refs[-1][index] = ref[...]

    return pl.pallas_call(
        body,
        name="stacked",
        in_specs=[IN_VMEM] * len(arrays),
        out_specs=IN_VMEM,
        out_shape=jax.ShapeDtypeStruct((len(arrays), *arrays[0].shape), arrays[0].dtype),
        compiler_params=pltpu.CompilerParams(vmem_limit_bytes=KERNEL_VMEM),
        cost_estimate=pl.CostEstimate(flops=10**8, bytes_accessed=10**6, transcendentals=0),
    )(*arrays)


def attend(query, blocks, index, marks=None):
    rows = query.shape[0]
    head = query.shape[1] // HEAD_DEV
    wide = 2 * head
    count = len(blocks)
    lines = rows // wide
    span = count * rows
    scale = head ** -0.5 * math.log2(math.e)
    first = marks is None
    kept = -(-count * lines // 8) * 8

    def body(*refs):
        q_ref, block_refs = refs[0], refs[1:1 + count]
        if first:
            out_ref, marks_ref, score_ref = refs[1 + count:]
            pieces = [ref[rows:rows + lines, :].astype(jnp.float32) for ref in block_refs]
            pieces.append(jnp.zeros((kept - count * lines, wide), jnp.float32))
            marks_ref[...] = jnp.concatenate(pieces, axis=0)
        else:
            marks_ref, out_ref, score_ref = refs[1 + count:]
        own = [jnp.broadcast_to(marks_ref[i:i + 1, :], (head, wide)) for i in range(lines)]
        own = jnp.concatenate([jnp.transpose(row) for row in own], axis=0)
        for start in range(0, rows, QUERY_TILE):
            tile = slice(start, start + QUERY_TILE)
            q_tile = q_ref[tile, index * head:(index + 1) * head]
            q_mark = own[tile, :]
            q_mark = jnp.concatenate([q_mark] * 2, axis=1)
            peak = None
            for piece in range(count * lines):
                block, offset = block_refs[piece // lines], piece % lines * wide
                score = lax.dot_general(
                    q_tile, block[offset:offset + wide, :head], (((1,), (1,)), ((), ())),
                    preferred_element_type=jnp.float32,
                )
                score = jnp.where(q_mark == marks_ref[piece:piece + 1, :], score, -1e30)
                score_ref[:, piece * wide:(piece + 1) * wide] = score
                largest = jnp.maximum(score[:, :head], score[:, head:])
                peak = largest if peak is None else jnp.maximum(peak, largest)
            peak = jnp.max(peak, axis=1, keepdims=True)
            summed, total = None, None
            for piece in range(count * lines):
                block, offset = block_refs[piece // lines], piece % lines * wide
                weight = jnp.exp2((score_ref[:, piece * wide:(piece + 1) * wide] - peak) * scale)
                folded = weight[:, :head] + weight[:, head:]
                term = jnp.dot(
                    weight.astype(jnp.bfloat16), block[offset:offset + wide, head:],
                    preferred_element_type=jnp.float32,
                )
                total = folded if total is None else total + folded
                summed = term if summed is None else summed + term
            total = jnp.sum(total, axis=1, keepdims=True)
            out_ref[tile, :] = (summed / total).astype(jnp.bfloat16)

    outs = [jax.ShapeDtypeStruct((rows, head), jnp.bfloat16)]
    if first:
        outs.append(jax.ShapeDtypeStruct((kept, wide), jnp.float32))
    result = pl.pallas_call(
        body,
        name="attend",
        in_specs=[IN_VMEM] * (1 + count + (not first)),
        out_specs=[IN_VMEM] * len(outs),
        out_shape=outs,
        scratch_shapes=[pltpu.VMEM((QUERY_TILE, span), jnp.float32)],
        compiler_params=pltpu.CompilerParams(vmem_limit_bytes=KERNEL_VMEM),
        cost_estimate=pl.CostEstimate(
            flops=8 * rows * span * head, bytes_accessed=4 * span * head, transcendentals=rows * span
        ),
    )(query, *blocks, *([] if first else [marks]))
    return result if first else [result[0], marks]


def assemble(order, own, pieces):
    groups, part, columns = pieces[0].shape
    count = len(pieces)

    def body(order_ref, own_ref, *refs):
        out_ref = refs[-1]
        out_ref[0] = own_ref[...]
        for index, ref in enumerate(refs[:-1]):
            place = pl.multiple_of((order_ref[0] ^ index) * part, part)
            out_ref[1:, pl.ds(place, part), :] = ref[...]

    return pl.pallas_call(
        body,
        name="assemble",
        in_specs=[pl.BlockSpec(memory_space=pltpu.SMEM)] + [IN_VMEM] * (count + 1),
        out_specs=IN_VMEM,
        out_shape=jax.ShapeDtypeStruct((groups + 1, part * count, columns), jnp.bfloat16),
        compiler_params=pltpu.CompilerParams(vmem_limit_bytes=KERNEL_VMEM),
        cost_estimate=pl.CostEstimate(
            flops=10**9, bytes_accessed=4 * groups * part * count * columns, transcendentals=0
        ),
    )(order, own, *pieces)


def tiles(columns):
    tile = 256 if columns % 256 == 0 else columns
    return [slice(start, start + tile) for start in range(0, columns, tile)]


def placed(left_ref, refs, parts):
    place = 0
    refs = iter(refs)
    for arrays in parts:
        value = functools.reduce(jnp.add, [next(refs)[...] for _ in arrays])
        left_ref[:, place:place + value.shape[1]] = value
        place += value.shape[1]


def project_first(weight, own, others):
    groups, depth, columns = weight.shape
    rows, head = own[0].shape
    parts = [[array] for array in own] + others
    flat = [array for arrays in parts for array in arrays]

    def body(w_ref, *refs):
        ins, out_ref, left_ref = refs[:len(flat)], refs[-2], refs[-1]
        placed(left_ref, ins, parts)
        for tile in tiles(columns):
            out = jnp.dot(left_ref[:, :depth], w_ref[0, :, tile], preferred_element_type=jnp.float32)
            for g in range(1, groups):
                place = depth + (g - 1) * head
                out += jnp.dot(
                    left_ref[:, place:place + head], w_ref[g, :head, tile],
                    preferred_element_type=jnp.float32,
                )
            out_ref[:, tile] = out

    return pl.pallas_call(
        body,
        name="project_first",
        in_specs=[IN_VMEM] * (1 + len(flat)),
        out_specs=IN_VMEM,
        out_shape=jax.ShapeDtypeStruct((rows, columns), jnp.float32),
        scratch_shapes=[pltpu.VMEM((rows, depth + (groups - 1) * head), jnp.bfloat16)],
        compiler_params=pltpu.CompilerParams(vmem_limit_bytes=KERNEL_VMEM),
        cost_estimate=pl.CostEstimate(
            flops=rows * groups * depth * columns, bytes_accessed=4 * columns * rows, transcendentals=0
        ),
    )(weight, *flat)


def project_last(weight, partial, others):
    groups, depth, columns = weight.shape
    rows, head = others[0][0].shape
    flat = [array for arrays in others for array in arrays]
    span = (groups - 1) * (depth - head)
    cuts = tiles(columns)

    def body(w_ref, p_ref, *refs):
        ins, (out_ref, left_ref, right_ref, done_ref, sems) = refs[:len(flat)], refs[len(flat):]
        placed(left_ref, ins, others)
        for g in range(1, groups):
            place = (g - 1) * (depth - head)
            right_ref[place:place + depth - head, :] = w_ref[g, head:, :]
        copies = []
        for number, tile in enumerate(cuts):
            out = p_ref[:, tile] + jnp.dot(
                left_ref[...], right_ref[:, tile], preferred_element_type=jnp.float32
            )
            done_ref[:, tile] = out.astype(jnp.bfloat16)
            copies.append(pltpu.make_async_copy(done_ref.at[:, tile], out_ref.at[:, tile], sems.at[number]))
            copies[-1].start()
        for copy in copies:
            copy.wait()

    return pl.pallas_call(
        body,
        name="project_last",
        in_specs=[IN_VMEM] * (2 + len(flat)),
        out_specs=pl.BlockSpec(memory_space=pltpu.HBM),
        out_shape=jax.ShapeDtypeStruct((rows, columns), jnp.bfloat16),
        scratch_shapes=[
            pltpu.VMEM((rows, span), jnp.bfloat16),
            pltpu.VMEM((span, columns), jnp.bfloat16),
            pltpu.VMEM((rows, columns), jnp.bfloat16),
            pltpu.SemaphoreType.DMA((len(cuts),)),
        ],
        compiler_params=pltpu.CompilerParams(vmem_limit_bytes=2 * KERNEL_VMEM),
        cost_estimate=pl.CostEstimate(
            flops=rows * groups * depth * columns, bytes_accessed=4 * columns * rows, transcendentals=0
        ),
    )(weight, partial, *flat)


def shards(queries, keys, values, segment_ids, out_weight):
    groups = lax.axis_size("head")
    me = lax.axis_index("head")
    place = lax.axis_index("seq")
    replicas = 4
    mine = (place & 1) + 2 * ((place >> 2) & 1)
    part, columns = out_weight.shape[0] // replicas, out_weight.shape[1] // groups

    messages = pack(keys, values, segment_ids)

    aligned = columns % LANES == 0
    corners = [
        (mine * part, partner(me, distance, groups) * columns) for distance in range(1, groups)
    ]
    if aligned:
        table = jnp.stack([value for corner in corners for value in corner]).astype(jnp.int32)
        pieces = cut(out_weight, table, part, columns)
    else:
        pieces = [lax.dynamic_slice(out_weight, corner, (part, columns)) for corner in corners]

    near, far, beside = [], [], []
    for message in messages:
        near.append(from_far(message, "seq", 1))
        far.append(from_far(message, "seq", -1))
        beside.append(exchanged(message, "seq", 1))

    received = []
    for distance, piece in enumerate(pieces, 1):
        received.append(to_partner(piece, "head", distance))
    first = stacked(received)
    second = exchanged(first, "seq", 4)
    third = exchanged(first, "seq", 1)
    fourth = exchanged(second, "seq", 1)
    own, others, marks = [], [], None
    for index, message in enumerate(messages):
        across = exchanged(near[index], "seq", 1)
        blocks = (message, beside[index], near[index], far[index], across)
        done, marks = attend(queries, blocks, index, marks)
        own.append(done)
        if index in relays():
            two = lax.ppermute(done, "head", [(0, 2), (2, 0), (1, 3), (3, 1)])
            one = lax.ppermute(done, "head", [(0, 1), (1, 0), (2, 3), (3, 2)])
            inner = lax.ppermute(done, "head", [(1, 2), (2, 1)])
            outer = lax.ppermute(two, "head", [(1, 0), (2, 3)])
            others.append([[one], [two], [inner, outer]])
        else:
            line = []
            for distance in range(1, groups):
                line.append([to_partner(done, "head", distance)])
            others.append(line)

    if aligned:
        table = jnp.stack([jnp.int32(0), (me * columns).astype(jnp.int32)])
        own_weight = cut(out_weight, table, out_weight.shape[0], columns)[0]
    else:
        own_weight = lax.dynamic_slice(out_weight, (0, me * columns), (out_weight.shape[0], columns))
    weight = assemble(mine.astype(jnp.int32)[None], own_weight, [first, third, second, fourth])
    partial = project_first(weight, own, others[0])
    rest = [line[distance] for distance in range(groups - 1) for line in others[1:]]
    return project_last(weight, partial, rest)


def solution(mesh):
    placed = (P("seq", "head"), P("seq", "head"), P("seq", "head"), P("seq"), P("head", None))
    return jax.shard_map(shards, mesh=mesh, in_specs=placed, out_specs=P("seq", "head"), check_vma=False)
```

```python
import functools
import math

import jax
import jax.numpy as jnp
from jax import lax
from jax.experimental import pallas as pl
from jax.experimental.pallas import tpu as pltpu
from jax.sharding import PartitionSpec as P

HEAD_DEV = 2
QUERY_TILE = 256
PAD_ROWS = 16
KERNEL_VMEM = 12 * 2**20
IN_VMEM = pl.BlockSpec(memory_space=pltpu.VMEM)
IN_HBM = pl.BlockSpec(memory_space=pltpu.HBM)
LANES = 128


def in_hbm(array):
    return pltpu.with_memory_space_constraint(array, pltpu.HBM)


def partner(index, distance, count):
    return index ^ distance if count & (count - 1) == 0 else (index + distance) % count


def to_partner(block, axis, distance):
    count = lax.axis_size(axis)
    return lax.ppermute(block, axis, [(i, partner(i, distance, count)) for i in range(count)])


def relays():
    return ()


def exchanged(block, axis, flip):
    return lax.ppermute(block, axis, [(i, i ^ flip) for i in range(lax.axis_size(axis))])


def from_far(block, axis, toward):
    count = lax.axis_size(axis)
    route = [(i + toward * (2 if i % 2 == 0 else -2), i) for i in range(count)]
    return lax.ppermute(block, axis, [(s, d) for s, d in route if 0 <= s < count])


def pack(keys, values, segment_ids):
    rows, width = keys.shape
    head = width // HEAD_DEV
    wide = 2 * head
    lines = rows // wide

    def body(k_ref, v_ref, s_ref, *refs):
        messages, (ids_ref, sems) = refs[:HEAD_DEV], refs[HEAD_DEV:]
        copies = [pltpu.make_async_copy(s_ref, ids_ref, sems.at[0])]
        for index, ref in enumerate(messages):
            for side, source in enumerate((k_ref, v_ref)):
                copies.append(pltpu.make_async_copy(
                    source.at[:, index * head:(index + 1) * head],
                    ref.at[:rows, side * head:(side + 1) * head],
                    sems.at[1 + 2 * index + side],
                ))
        for copy in copies:
            copy.start()
        copies[0].wait()
        marks = (ids_ref[...] + 1).astype(jnp.float32)
        parts = [marks[:, i * wide:(i + 1) * wide] for i in range(lines)]
        parts.append(jnp.zeros((PAD_ROWS - lines, wide), jnp.float32))
        messages[0][rows:, :] = jnp.concatenate(parts, axis=0).astype(jnp.bfloat16)
        for copy in copies[1:]:
            copy.wait()

    shapes = [(rows + PAD_ROWS, wide)] + [(rows, wide)] * (HEAD_DEV - 1)
    return pl.pallas_call(
        body,
        name="pack",
        in_specs=[IN_HBM] * 3,
        out_specs=[IN_VMEM] * HEAD_DEV,
        out_shape=[jax.ShapeDtypeStruct(shape, jnp.bfloat16) for shape in shapes],
        scratch_shapes=[
            pltpu.VMEM((1, rows), jnp.int32), pltpu.SemaphoreType.DMA((1 + 2 * HEAD_DEV,)),
        ],
        compiler_params=pltpu.CompilerParams(vmem_limit_bytes=KERNEL_VMEM),
        cost_estimate=pl.CostEstimate(flops=10**9, bytes_accessed=8 * rows * width, transcendentals=0),
    )(*[in_hbm(x) for x in (keys, values, segment_ids.reshape(1, rows))])


def cut(array, corners, rows, columns):
    count = corners.shape[0] // 2

    def body(corner_ref, source_ref, *refs):
        copies = []
        for index in range(count):
            row = pl.multiple_of(corner_ref[2 * index], rows)
            column = pl.multiple_of(corner_ref[2 * index + 1], columns)
            copies.append(pltpu.make_async_copy(
                source_ref.at[pl.ds(row, rows), pl.ds(column, columns)], refs[index], refs[-1].at[index]
            ))
        for copy in copies:
            copy.start()
        for copy in copies:
            copy.wait()

    return pl.pallas_call(
        body,
        name="cut",
        in_specs=[pl.BlockSpec(memory_space=pltpu.SMEM), IN_HBM],
        out_specs=[IN_VMEM] * count,
        out_shape=[jax.ShapeDtypeStruct((rows, columns), array.dtype)] * count,
        scratch_shapes=[pltpu.SemaphoreType.DMA((count,))],
        compiler_params=pltpu.CompilerParams(vmem_limit_bytes=KERNEL_VMEM),
        cost_estimate=pl.CostEstimate(
            flops=10**9, bytes_accessed=4 * count * rows * columns, transcendentals=0
        ),
    )(corners, in_hbm(array))


def stacked(arrays):
    def body(*refs):
        for index, ref in enumerate(refs[:-1]):
            refs[-1][index] = ref[...]

    return pl.pallas_call(
        body,
        name="stacked",
        in_specs=[IN_VMEM] * len(arrays),
        out_specs=IN_VMEM,
        out_shape=jax.ShapeDtypeStruct((len(arrays), *arrays[0].shape), arrays[0].dtype),
        compiler_params=pltpu.CompilerParams(vmem_limit_bytes=KERNEL_VMEM),
        cost_estimate=pl.CostEstimate(flops=10**8, bytes_accessed=10**6, transcendentals=0),
    )(*arrays)


def attend(query, blocks, index, marks=None):
    rows = query.shape[0]
    head = query.shape[1] // HEAD_DEV
    wide = 2 * head
    count = len(blocks)
    lines = rows // wide
    span = count * rows
    scale = head ** -0.5 * math.log2(math.e)
    first = marks is None
    kept = -(-count * lines // 8) * 8

    def body(*refs):
        q_ref, block_refs = refs[0], refs[1:1 + count]
        if first:
            out_ref, marks_ref, score_ref = refs[1 + count:]
            pieces = [ref[rows:rows + lines, :].astype(jnp.float32) for ref in block_refs]
            pieces.append(jnp.zeros((kept - count * lines, wide), jnp.float32))
            marks_ref[...] = jnp.concatenate(pieces, axis=0)
        else:
            marks_ref, out_ref, score_ref = refs[1 + count:]
        own = [jnp.broadcast_to(marks_ref[i:i + 1, :], (head, wide)) for i in range(lines)]
        own = jnp.concatenate([jnp.transpose(row) for row in own], axis=0)
        for start in range(0, rows, QUERY_TILE):
            tile = slice(start, start + QUERY_TILE)
            q_tile = q_ref[tile, index * head:(index + 1) * head]
            q_mark = own[tile, :]
            q_mark = jnp.concatenate([q_mark] * 2, axis=1)
            peak = None
            for piece in range(count * lines):
                block, offset = block_refs[piece // lines], piece % lines * wide
                score = lax.dot_general(
                    q_tile, block[offset:offset + wide, :head], (((1,), (1,)), ((), ())),
                    preferred_element_type=jnp.float32,
                )
                score = jnp.where(q_mark == marks_ref[piece:piece + 1, :], score, -1e30)
                score_ref[:, piece * wide:(piece + 1) * wide] = score
                largest = jnp.maximum(score[:, :head], score[:, head:])
                peak = largest if peak is None else jnp.maximum(peak, largest)
            peak = jnp.max(peak, axis=1, keepdims=True)
            summed, total = None, None
            for piece in range(count * lines):
                block, offset = block_refs[piece // lines], piece % lines * wide
                weight = jnp.exp2((score_ref[:, piece * wide:(piece + 1) * wide] - peak) * scale)
                folded = weight[:, :head] + weight[:, head:]
                term = jnp.dot(
                    weight.astype(jnp.bfloat16), block[offset:offset + wide, head:],
                    preferred_element_type=jnp.float32,
                )
                total = folded if total is None else total + folded
                summed = term if summed is None else summed + term
            total = jnp.sum(total, axis=1, keepdims=True)
            out_ref[tile, :] = (summed / total).astype(jnp.bfloat16)

    outs = [jax.ShapeDtypeStruct((rows, head), jnp.bfloat16)]
    if first:
        outs.append(jax.ShapeDtypeStruct((kept, wide), jnp.float32))
    result = pl.pallas_call(
        body,
        name="attend",
        in_specs=[IN_VMEM] * (1 + count + (not first)),
        out_specs=[IN_VMEM] * len(outs),
        out_shape=outs,
        scratch_shapes=[pltpu.VMEM((QUERY_TILE, span), jnp.float32)],
        compiler_params=pltpu.CompilerParams(vmem_limit_bytes=KERNEL_VMEM),
        cost_estimate=pl.CostEstimate(
            flops=8 * rows * span * head, bytes_accessed=4 * span * head, transcendentals=rows * span
        ),
    )(query, *blocks, *([] if first else [marks]))
    return result if first else [result[0], marks]


def assemble(order, own, pieces):
    groups, part, columns = pieces[0].shape
    count = len(pieces)

    def body(order_ref, own_ref, *refs):
        out_ref = refs[-1]
        out_ref[0] = own_ref[...]
        for index, ref in enumerate(refs[:-1]):
            place = pl.multiple_of((order_ref[0] ^ index) * part, part)
            out_ref[1:, pl.ds(place, part), :] = ref[...]

    return pl.pallas_call(
        body,
        name="assemble",
        in_specs=[pl.BlockSpec(memory_space=pltpu.SMEM)] + [IN_VMEM] * (count + 1),
        out_specs=IN_VMEM,
        out_shape=jax.ShapeDtypeStruct((groups + 1, part * count, columns), jnp.bfloat16),
        compiler_params=pltpu.CompilerParams(vmem_limit_bytes=KERNEL_VMEM),
        cost_estimate=pl.CostEstimate(
            flops=10**9, bytes_accessed=4 * groups * part * count * columns, transcendentals=0
        ),
    )(order, own, *pieces)


def tiles(columns):
    tile = 256 if columns % 256 == 0 else columns
    return [slice(start, start + tile) for start in range(0, columns, tile)]


def placed(left_ref, refs, parts):
    place = 0
    refs = iter(refs)
    for arrays in parts:
        value = functools.reduce(jnp.add, [next(refs)[...] for _ in arrays])
        left_ref[:, place:place + value.shape[1]] = value
        place += value.shape[1]


def project_first(weight, own, others):
    groups, depth, columns = weight.shape
    rows, head = own[0].shape
    parts = [[array] for array in own] + others
    flat = [array for arrays in parts for array in arrays]

    def body(w_ref, *refs):
        ins, out_ref, left_ref = refs[:len(flat)], refs[-2], refs[-1]
        placed(left_ref, ins, parts)
        for tile in tiles(columns):
            out = jnp.dot(left_ref[:, :depth], w_ref[0, :, tile], preferred_element_type=jnp.float32)
            for g in range(1, groups):
                place = depth + (g - 1) * head
                out += jnp.dot(
                    left_ref[:, place:place + head], w_ref[g, :head, tile],
                    preferred_element_type=jnp.float32,
                )
            out_ref[:, tile] = out

    return pl.pallas_call(
        body,
        name="project_first",
        in_specs=[IN_VMEM] * (1 + len(flat)),
        out_specs=IN_VMEM,
        out_shape=jax.ShapeDtypeStruct((rows, columns), jnp.float32),
        scratch_shapes=[pltpu.VMEM((rows, depth + (groups - 1) * head), jnp.bfloat16)],
        compiler_params=pltpu.CompilerParams(vmem_limit_bytes=KERNEL_VMEM),
        cost_estimate=pl.CostEstimate(
            flops=rows * groups * depth * columns, bytes_accessed=4 * columns * rows, transcendentals=0
        ),
    )(weight, *flat)


def project_more(weight, partial, parts, last):
    _, _, columns = weight.shape
    rows, head = parts[0][0].shape
    cuts = tiles(columns)

    def body(w_ref, p_ref, *refs):
        ins, (out_ref, *rest) = refs[:len(parts)], refs[len(parts):]
        copies = []
        for number, tile in enumerate(cuts):
            out = p_ref[:, tile]
            for ref, (_, group, row) in zip(ins, parts):
                out += jnp.dot(
                    ref[...], w_ref[group, row:row + head, tile], preferred_element_type=jnp.float32
                )
            if not last:
                out_ref[:, tile] = out
                continue
            done_ref, sems = rest
            done_ref[:, tile] = out.astype(jnp.bfloat16)
            copies.append(pltpu.make_async_copy(done_ref.at[:, tile], out_ref.at[:, tile], sems.at[number]))
            copies[-1].start()
        for copy in copies:
            copy.wait()

    scratch = [pltpu.VMEM((rows, columns), jnp.bfloat16), pltpu.SemaphoreType.DMA((len(cuts),))]
    return pl.pallas_call(
        body,
        name="project_last" if last else "project_more",
        in_specs=[IN_VMEM] * (2 + len(parts)),
        out_specs=IN_HBM if last else IN_VMEM,
        out_shape=jax.ShapeDtypeStruct((rows, columns), jnp.bfloat16 if last else jnp.float32),
        scratch_shapes=scratch if last else [],
        compiler_params=pltpu.CompilerParams(vmem_limit_bytes=KERNEL_VMEM),
        cost_estimate=pl.CostEstimate(
            flops=2 * rows * len(parts) * head * columns, bytes_accessed=4 * columns * rows, transcendentals=0
        ),
    )(weight, partial, *[part[0] for part in parts])


def shards(queries, keys, values, segment_ids, out_weight):
    groups = lax.axis_size("head")
    me = lax.axis_index("head")
    place = lax.axis_index("seq")
    replicas = 4
    mine = (place & 1) + 2 * ((place >> 2) & 1)
    part, columns = out_weight.shape[0] // replicas, out_weight.shape[1] // groups

    messages = pack(keys, values, segment_ids)

    aligned = columns % LANES == 0
    corners = [
        (mine * part, partner(me, distance, groups) * columns) for distance in range(1, groups)
    ]
    if aligned:
        table = jnp.stack([value for corner in corners for value in corner]).astype(jnp.int32)
        pieces = cut(out_weight, table, part, columns)
    else:
        pieces = [lax.dynamic_slice(out_weight, corner, (part, columns)) for corner in corners]

    near, far, beside = [], [], []
    for message in messages:
        near.append(from_far(message, "seq", 1))
        far.append(from_far(message, "seq", -1))
        beside.append(exchanged(message, "seq", 1))

    received = []
    for distance, piece in enumerate(pieces, 1):
        received.append(to_partner(piece, "head", distance))
    first = stacked(received)
    second = exchanged(first, "seq", 4)
    third = exchanged(first, "seq", 1)
    fourth = exchanged(second, "seq", 1)
    own, others, marks = [], [], None
    for index, message in enumerate(messages):
        across = exchanged(near[index], "seq", 1)
        blocks = (message, beside[index], near[index], far[index], across)
        done, marks = attend(queries, blocks, index, marks)
        own.append(done)
        if index in relays():
            two = lax.ppermute(done, "head", [(0, 2), (2, 0), (1, 3), (3, 1)])
            one = lax.ppermute(done, "head", [(0, 1), (1, 0), (2, 3), (3, 2)])
            inner = lax.ppermute(done, "head", [(1, 2), (2, 1)])
            outer = lax.ppermute(two, "head", [(1, 0), (2, 3)])
            others.append([[one], [two], [inner, outer]])
        else:
            line = []
            for distance in range(1, groups):
                line.append([to_partner(done, "head", distance)])
            others.append(line)

    if aligned:
        table = jnp.stack([jnp.int32(0), (me * columns).astype(jnp.int32)])
        own_weight = cut(out_weight, table, out_weight.shape[0], columns)[0]
    else:
        own_weight = lax.dynamic_slice(out_weight, (0, me * columns), (out_weight.shape[0], columns))
    weight = assemble(mine.astype(jnp.int32)[None], own_weight, [first, third, second, fourth])
    partial = project_first(weight, own, others[0])
    head = queries.shape[1] // HEAD_DEV
    parts = [
        (line[distance - 1][0], distance, index * head)
        for distance in turns(groups) for index, line in enumerate(others) if index
    ]
    final = HEAD_DEV - 1
    if len(parts) > final:
        partial = project_more(weight, partial, parts[:-final], False)
    return project_more(weight, partial, parts[-final:], True)


def turns(groups):
    return [2, 1, 3] if groups == 4 else list(range(1, groups))


def solution(mesh):
    placed = (P("seq", "head"), P("seq", "head"), P("seq", "head"), P("seq"), P("head", None))
    return jax.shard_map(shards, mesh=mesh, in_specs=placed, out_specs=P("seq", "head"), check_vma=False)
```

```python
import functools
import math

import jax
import jax.numpy as jnp
from jax import lax
from jax.experimental import pallas as pl
from jax.experimental.pallas import tpu as pltpu
from jax.sharding import PartitionSpec as P

HEAD_DEV = 2
QUERY_TILE = 256
PAD_ROWS = 16
KERNEL_VMEM = 12 * 2**20
IN_VMEM = pl.BlockSpec(memory_space=pltpu.VMEM)
IN_HBM = pl.BlockSpec(memory_space=pltpu.HBM)
LANES = 128


def in_hbm(array):
    return pltpu.with_memory_space_constraint(array, pltpu.HBM)


def partner(index, distance, count):
    return index ^ distance if count & (count - 1) == 0 else (index + distance) % count


def to_partner(block, axis, distance):
    count = lax.axis_size(axis)
    return lax.ppermute(block, axis, [(i, partner(i, distance, count)) for i in range(count)])


def relays():
    return ()


def exchanged(block, axis, flip):
    return lax.ppermute(block, axis, [(i, i ^ flip) for i in range(lax.axis_size(axis))])


def from_far(block, axis, toward):
    count = lax.axis_size(axis)
    route = [(i + toward * (2 if i % 2 == 0 else -2), i) for i in range(count)]
    return lax.ppermute(block, axis, [(s, d) for s, d in route if 0 <= s < count])


def pack(keys, values, segment_ids, heads):
    rows, width = keys.shape
    head = width // HEAD_DEV
    wide = 2 * head
    lines = rows // wide

    def body(k_ref, v_ref, s_ref, *refs):
        messages, (ids_ref, sems) = refs[:len(heads)], refs[len(heads):]
        copies = [pltpu.make_async_copy(s_ref, ids_ref, sems.at[0])]
        for place, (index, ref) in enumerate(zip(heads, messages)):
            for side, source in enumerate((k_ref, v_ref)):
                copies.append(pltpu.make_async_copy(
                    source.at[:, index * head:(index + 1) * head],
                    ref.at[:rows, side * head:(side + 1) * head],
                    sems.at[1 + 2 * place + side],
                ))
        for copy in copies:
            copy.start()
        copies[0].wait()
        marks = (ids_ref[...] + 1).astype(jnp.float32)
        parts = [marks[:, i * wide:(i + 1) * wide] for i in range(lines)]
        parts.append(jnp.zeros((PAD_ROWS - lines, wide), jnp.float32))
        if 0 in heads:
            messages[0][rows:, :] = jnp.concatenate(parts, axis=0).astype(jnp.bfloat16)
        for copy in copies[1:]:
            copy.wait()

    shapes = [(rows if index else rows + PAD_ROWS, wide) for index in heads]
    return pl.pallas_call(
        body,
        name="pack",
        in_specs=[IN_HBM] * 3,
        out_specs=[IN_VMEM] * len(heads),
        out_shape=[jax.ShapeDtypeStruct(shape, jnp.bfloat16) for shape in shapes],
        scratch_shapes=[
            pltpu.VMEM((1, rows), jnp.int32), pltpu.SemaphoreType.DMA((1 + 2 * len(heads),)),
        ],
        compiler_params=pltpu.CompilerParams(vmem_limit_bytes=KERNEL_VMEM),
        cost_estimate=pl.CostEstimate(flops=10**9, bytes_accessed=8 * rows * width, transcendentals=0),
    )(*[in_hbm(x) for x in (keys, values, segment_ids.reshape(1, rows))])


def cut(array, corners, rows, columns):
    count = corners.shape[0] // 2

    def body(corner_ref, source_ref, *refs):
        copies = []
        for index in range(count):
            row = pl.multiple_of(corner_ref[2 * index], rows)
            column = pl.multiple_of(corner_ref[2 * index + 1], columns)
            copies.append(pltpu.make_async_copy(
                source_ref.at[pl.ds(row, rows), pl.ds(column, columns)], refs[index], refs[-1].at[index]
            ))
        for copy in copies:
            copy.start()
        for copy in copies:
            copy.wait()

    return pl.pallas_call(
        body,
        name="cut",
        in_specs=[pl.BlockSpec(memory_space=pltpu.SMEM), IN_HBM],
        out_specs=[IN_VMEM] * count,
        out_shape=[jax.ShapeDtypeStruct((rows, columns), array.dtype)] * count,
        scratch_shapes=[pltpu.SemaphoreType.DMA((count,))],
        compiler_params=pltpu.CompilerParams(vmem_limit_bytes=KERNEL_VMEM),
        cost_estimate=pl.CostEstimate(
            flops=10**9, bytes_accessed=4 * count * rows * columns, transcendentals=0
        ),
    )(corners, in_hbm(array))


def stacked(arrays):
    def body(*refs):
        for index, ref in enumerate(refs[:-1]):
            refs[-1][index] = ref[...]

    return pl.pallas_call(
        body,
        name="stacked",
        in_specs=[IN_VMEM] * len(arrays),
        out_specs=IN_VMEM,
        out_shape=jax.ShapeDtypeStruct((len(arrays), *arrays[0].shape), arrays[0].dtype),
        compiler_params=pltpu.CompilerParams(vmem_limit_bytes=KERNEL_VMEM),
        cost_estimate=pl.CostEstimate(flops=10**8, bytes_accessed=10**6, transcendentals=0),
    )(*arrays)


def attend(query, blocks, index, marks=None):
    rows = query.shape[0]
    head = query.shape[1] // HEAD_DEV
    wide = 2 * head
    count = len(blocks)
    lines = rows // wide
    span = count * rows
    scale = head ** -0.5 * math.log2(math.e)
    first = marks is None
    kept = -(-count * lines // 8) * 8

    def body(*refs):
        q_ref, block_refs = refs[0], refs[1:1 + count]
        if first:
            out_ref, marks_ref, score_ref = refs[1 + count:]
            pieces = [ref[rows:rows + lines, :].astype(jnp.float32) for ref in block_refs]
            pieces.append(jnp.zeros((kept - count * lines, wide), jnp.float32))
            marks_ref[...] = jnp.concatenate(pieces, axis=0)
        else:
            marks_ref, out_ref, score_ref = refs[1 + count:]
        own = [jnp.broadcast_to(marks_ref[i:i + 1, :], (head, wide)) for i in range(lines)]
        own = jnp.concatenate([jnp.transpose(row) for row in own], axis=0)
        for start in range(0, rows, QUERY_TILE):
            tile = slice(start, start + QUERY_TILE)
            q_tile = q_ref[tile, index * head:(index + 1) * head]
            q_mark = own[tile, :]
            q_mark = jnp.concatenate([q_mark] * 2, axis=1)
            peak = None
            for piece in range(count * lines):
                block, offset = block_refs[piece // lines], piece % lines * wide
                score = lax.dot_general(
                    q_tile, block[offset:offset + wide, :head], (((1,), (1,)), ((), ())),
                    preferred_element_type=jnp.float32,
                )
                score = jnp.where(q_mark == marks_ref[piece:piece + 1, :], score, -1e30)
                score_ref[:, piece * wide:(piece + 1) * wide] = score
                largest = jnp.maximum(score[:, :head], score[:, head:])
                peak = largest if peak is None else jnp.maximum(peak, largest)
            peak = jnp.max(peak, axis=1, keepdims=True)
            summed, total = None, None
            for piece in range(count * lines):
                block, offset = block_refs[piece // lines], piece % lines * wide
                weight = jnp.exp2((score_ref[:, piece * wide:(piece + 1) * wide] - peak) * scale)
                folded = weight[:, :head] + weight[:, head:]
                term = jnp.dot(
                    weight.astype(jnp.bfloat16), block[offset:offset + wide, head:],
                    preferred_element_type=jnp.float32,
                )
                total = folded if total is None else total + folded
                summed = term if summed is None else summed + term
            total = jnp.sum(total, axis=1, keepdims=True)
            out_ref[tile, :] = (summed / total).astype(jnp.bfloat16)

    outs = [jax.ShapeDtypeStruct((rows, head), jnp.bfloat16)]
    if first:
        outs.append(jax.ShapeDtypeStruct((kept, wide), jnp.float32))
    result = pl.pallas_call(
        body,
        name="attend",
        in_specs=[IN_VMEM] * (1 + count + (not first)),
        out_specs=[IN_VMEM] * len(outs),
        out_shape=outs,
        scratch_shapes=[pltpu.VMEM((QUERY_TILE, span), jnp.float32)],
        compiler_params=pltpu.CompilerParams(vmem_limit_bytes=KERNEL_VMEM),
        cost_estimate=pl.CostEstimate(
            flops=8 * rows * span * head, bytes_accessed=4 * span * head, transcendentals=rows * span
        ),
    )(query, *blocks, *([] if first else [marks]))
    return result if first else [result[0], marks]


def assemble(order, own, pieces):
    groups, part, columns = pieces[0].shape
    count = len(pieces)

    def body(order_ref, own_ref, *refs):
        out_ref = refs[-1]
        out_ref[0] = own_ref[...]
        for index, ref in enumerate(refs[:-1]):
            place = pl.multiple_of((order_ref[0] ^ index) * part, part)
            out_ref[1:, pl.ds(place, part), :] = ref[...]

    return pl.pallas_call(
        body,
        name="assemble",
        in_specs=[pl.BlockSpec(memory_space=pltpu.SMEM)] + [IN_VMEM] * (count + 1),
        out_specs=IN_VMEM,
        out_shape=jax.ShapeDtypeStruct((groups + 1, part * count, columns), jnp.bfloat16),
        compiler_params=pltpu.CompilerParams(vmem_limit_bytes=KERNEL_VMEM),
        cost_estimate=pl.CostEstimate(
            flops=10**9, bytes_accessed=4 * groups * part * count * columns, transcendentals=0
        ),
    )(order, own, *pieces)


def tiles(columns):
    tile = 256 if columns % 256 == 0 else columns
    return [slice(start, start + tile) for start in range(0, columns, tile)]


def placed(left_ref, refs, parts):
    place = 0
    refs = iter(refs)
    for arrays in parts:
        value = functools.reduce(jnp.add, [next(refs)[...] for _ in arrays])
        left_ref[:, place:place + value.shape[1]] = value
        place += value.shape[1]


def project_first(weight, own, others):
    groups, depth, columns = weight.shape
    rows, head = own[0].shape
    parts = [[array] for array in own] + others
    flat = [array for arrays in parts for array in arrays]

    def body(w_ref, *refs):
        ins, out_ref, left_ref = refs[:len(flat)], refs[-2], refs[-1]
        placed(left_ref, ins, parts)
        for tile in tiles(columns):
            out = jnp.dot(left_ref[:, :depth], w_ref[0, :, tile], preferred_element_type=jnp.float32)
            for g in range(1, groups):
                place = depth + (g - 1) * head
                out += jnp.dot(
                    left_ref[:, place:place + head], w_ref[g, :head, tile],
                    preferred_element_type=jnp.float32,
                )
            out_ref[:, tile] = out

    return pl.pallas_call(
        body,
        name="project_first",
        in_specs=[IN_VMEM] * (1 + len(flat)),
        out_specs=IN_VMEM,
        out_shape=jax.ShapeDtypeStruct((rows, columns), jnp.float32),
        scratch_shapes=[pltpu.VMEM((rows, depth + (groups - 1) * head), jnp.bfloat16)],
        compiler_params=pltpu.CompilerParams(vmem_limit_bytes=KERNEL_VMEM),
        cost_estimate=pl.CostEstimate(
            flops=rows * groups * depth * columns, bytes_accessed=4 * columns * rows, transcendentals=0
        ),
    )(weight, *flat)


def project_more(weight, partial, parts, last):
    _, _, columns = weight.shape
    rows, head = parts[0][0].shape
    cuts = tiles(columns)

    def body(w_ref, p_ref, *refs):
        ins, (out_ref, *rest) = refs[:len(parts)], refs[len(parts):]
        copies = []
        for number, tile in enumerate(cuts):
            out = p_ref[:, tile]
            for ref, (_, group, row) in zip(ins, parts):
                out += jnp.dot(
                    ref[...], w_ref[group, row:row + head, tile], preferred_element_type=jnp.float32
                )
            if not last:
                out_ref[:, tile] = out
                continue
            done_ref, sems = rest
            done_ref[:, tile] = out.astype(jnp.bfloat16)
            copies.append(pltpu.make_async_copy(done_ref.at[:, tile], out_ref.at[:, tile], sems.at[number]))
            copies[-1].start()
        for copy in copies:
            copy.wait()

    scratch = [pltpu.VMEM((rows, columns), jnp.bfloat16), pltpu.SemaphoreType.DMA((len(cuts),))]
    return pl.pallas_call(
        body,
        name="project_last" if last else "project_more",
        in_specs=[IN_VMEM] * (2 + len(parts)),
        out_specs=IN_HBM if last else IN_VMEM,
        out_shape=jax.ShapeDtypeStruct((rows, columns), jnp.bfloat16 if last else jnp.float32),
        scratch_shapes=scratch if last else [],
        compiler_params=pltpu.CompilerParams(vmem_limit_bytes=KERNEL_VMEM),
        cost_estimate=pl.CostEstimate(
            flops=2 * rows * len(parts) * head * columns, bytes_accessed=4 * columns * rows, transcendentals=0
        ),
    )(weight, partial, *[part[0] for part in parts])


def shards(queries, keys, values, segment_ids, out_weight):
    groups = lax.axis_size("head")
    me = lax.axis_index("head")
    place = lax.axis_index("seq")
    replicas = 4
    mine = (place & 1) + 2 * ((place >> 2) & 1)
    part, columns = out_weight.shape[0] // replicas, out_weight.shape[1] // groups

    messages = pack(keys, values, segment_ids, [0])
    messages = [*messages, *pack(keys, values, segment_ids, list(range(1, HEAD_DEV)))]

    aligned = columns % LANES == 0
    corners = [
        (mine * part, partner(me, distance, groups) * columns) for distance in range(1, groups)
    ]
    if aligned:
        table = jnp.stack([value for corner in corners for value in corner]).astype(jnp.int32)
        pieces = cut(out_weight, table, part, columns)
    else:
        pieces = [lax.dynamic_slice(out_weight, corner, (part, columns)) for corner in corners]

    near, far, beside = [], [], []
    for message in messages:
        near.append(from_far(message, "seq", 1))
        far.append(from_far(message, "seq", -1))
        beside.append(exchanged(message, "seq", 1))

    received = []
    for distance, piece in enumerate(pieces, 1):
        received.append(to_partner(piece, "head", distance))
    first = stacked(received)
    second = exchanged(first, "seq", 4)
    third = exchanged(first, "seq", 1)
    fourth = exchanged(second, "seq", 1)
    own, others, marks = [], [], None
    for index, message in enumerate(messages):
        across = exchanged(near[index], "seq", 1)
        blocks = (message, beside[index], near[index], far[index], across)
        done, marks = attend(queries, blocks, index, marks)
        own.append(done)
        if index in relays():
            two = lax.ppermute(done, "head", [(0, 2), (2, 0), (1, 3), (3, 1)])
            one = lax.ppermute(done, "head", [(0, 1), (1, 0), (2, 3), (3, 2)])
            inner = lax.ppermute(done, "head", [(1, 2), (2, 1)])
            outer = lax.ppermute(two, "head", [(1, 0), (2, 3)])
            others.append([[one], [two], [inner, outer]])
        else:
            line = []
            for distance in range(1, groups):
                line.append([to_partner(done, "head", distance)])
            others.append(line)

    if aligned:
        table = jnp.stack([jnp.int32(0), (me * columns).astype(jnp.int32)])
        own_weight = cut(out_weight, table, out_weight.shape[0], columns)[0]
    else:
        own_weight = lax.dynamic_slice(out_weight, (0, me * columns), (out_weight.shape[0], columns))
    weight = assemble(mine.astype(jnp.int32)[None], own_weight, [first, third, second, fourth])
    partial = project_first(weight, own, others[0])
    head = queries.shape[1] // HEAD_DEV
    parts = [
        (line[distance - 1][0], distance, index * head)
        for distance in turns(groups) for index, line in enumerate(others) if index
    ]
    final = HEAD_DEV - 1
    if len(parts) > final:
        partial = project_more(weight, partial, parts[:-final], False)
    return project_more(weight, partial, parts[-final:], True)


def turns(groups):
    return [2, 1, 3] if groups == 4 else list(range(1, groups))


def solution(mesh):
    placed = (P("seq", "head"), P("seq", "head"), P("seq", "head"), P("seq"), P("head", None))
    return jax.shard_map(shards, mesh=mesh, in_specs=placed, out_specs=P("seq", "head"), check_vma=False)
```
